32 devices in a mesh: grp: 8 (over y, x, core), dom: 4 (over z).
Axes of the slice: x: 2, y: 2, z: 4, core: 2. Of those that a mesh axis runs over, the one named last changes fastest.
Arguments:
- surplus: float32 [128, 512, 512], P('grp', 'dom'), may hold values from -0.4 to 0.4
- block_ids: int32 [128, 512], P('grp', 'dom'), may hold values from 0 to 4095, as said below
- coef: int32 [128], P('grp'), may hold values from -4 to 6, as said below
Outputs:
- updated: float32 [128, 512, 512], P('grp', 'dom')
The draws below stay inside these ranges and needn't reach their ends.
Inputs may be any that keep to these rules, and one draw needn't show every extreme that they name: `block_ids`: for each grid, the slots in columns d * 128 to (d + 1) * 128 - 1 hold 128 different numbers from d * 1024 to (d + 1) * 1024 - 1. `coef`: each coefficient is one of 1, -4, 6.
All inputs are finite; a program needn't handle non-finite values.
Results may differ from the reference program's by a relative error of at most 0.000071.
Values sent between devices are 32-bit elements; how exact they have to be, the bound alone decides.
A program may use at most 64 MiB of HBM per device.

```python
import jax
import jax.numpy as jnp

K = 128
NBD = 1024
BLK = 512
GRIDS = 128
BLOCKS = 4096
N_DOM = 4


def draw_block_ids(key, part):
    keys = jax.random.split(jax.random.fold_in(key, 11), GRIDS * N_DOM)
    picked = jax.vmap(lambda single: jax.random.permutation(single, NBD)[:K])(keys)
    picked = picked.reshape(GRIDS, N_DOM, K).astype(jnp.int32)
    offsets = (jnp.arange(N_DOM, dtype=jnp.int32) * NBD)[None, :, None]
    return (picked + offsets).reshape(GRIDS, N_DOM * K)


def draw_coef(key, part):
    picks = jax.random.randint(jax.random.fold_in(key, 23), (GRIDS,), 0, 5)
    table = jnp.array([1, -4, 6, -4, 1], jnp.int32)
    return table[picks]


def steps_of(own_key, shape, shards, least, top_value):
    factor_of, own = 1.0, jax.random.fold_in(own_key, 6)
    for position, parts in shards:
        steps = jnp.exp(jax.random.uniform(jax.random.fold_in(own, position), (parts,), jnp.float32, least / len(shards), top_value / len(shards)))
        factor_of = factor_of * jnp.repeat(steps, shape[position] // parts).reshape([-1 if axis == position else 1 for axis in range(len(shape))])
    return factor_of


def normal_values(rng, dims, width, bound, shards=(), held_as=jnp.bfloat16):
    loudness = steps_of(rng, dims, shards, -0.22, 0.18) if shards else 1.0
    result = jax.random.normal(rng, dims, jnp.float32) * width * loudness
    return jnp.minimum(jnp.maximum(result, -bound), bound).astype(held_as)


def setup_inputs(seed: int = 0) -> dict:
    splits = jax.random.split(jax.random.key(seed), 4)
    return {
        "surplus": normal_values(splits[0], (GRIDS, N_DOM * K, BLK), 0.05, 0.4, ((0, 8), (1, 4)), jnp.float32),
        "block_ids": draw_block_ids(jax.random.fold_in(splits[3], 71), 0),
        "coef": draw_coef(jax.random.fold_in(splits[3], 71), 0),
    }


def reference(surplus, block_ids, coef):
    scaled = surplus * coef.astype(jnp.float32)[:, None, None]
    flat_ids = block_ids.reshape(-1).astype(jnp.int32)
    combined = jnp.zeros((BLOCKS, BLK), jnp.float32)
    combined = combined.at[flat_ids].add(scaled.reshape(-1, BLK))
    return combined[block_ids]
```

```python
import functools

import jax
import jax.numpy as jnp
from jax import lax
from jax.experimental import pallas as pl
from jax.experimental.pallas import tpu as pltpu
from jax.sharding import PartitionSpec as P

NBD = 1024
CORES = 2
SIDE = 2
STREAMS = 2
LOADS = 4
MESH = pl.DeviceIdType.MESH
DIAG, XN, YN, OWN = 0, 1, 2, 3
F32, BF16 = jnp.float32, jnp.bfloat16


def kernel(ids_ref, coef_ref, x_ref, out_ref, xf, xhi, xlo, w, oh, p, rd, rrel,
           rx, ry, cc, chi, clo, idst, load_sem, ss, rs):
    grids, k, blk = x_ref.shape
    part = rd.shape[1]
    rows = part // STREAMS
    h = rows // 2
    per = grids // LOADS

    me = lax.axis_index("grp")
    core = lax.rem(me, CORES)
    chip = me // CORES
    x, y = lax.rem(chip, SIDE), chip // SIDE
    ox, oy = 1 - x, 1 - y

    def index_of(cy, cx):
        return cy * SIDE + cx

    chips = {DIAG: index_of(oy, ox), XN: index_of(y, ox), YN: index_of(oy, x), OWN: chip}
    partner = chip * CORES + (1 - core)
    xn, yn = chips[XN] * CORES + core, chips[YN] * CORES + core
    origin = lax.axis_index("dom") * NBD

    def base(q, other):
        c = 1 - core if other else core
        return origin + (chips[q] * CORES + c) * part

    loads = []
    for n in range(LOADS):
        span = pl.ds(n * per, per)
        copy = pltpu.make_async_copy(x_ref.at[span], xf.at[span], load_sem.at[n])
        copy.start()
        loads.append(copy)

    barrier = pltpu.get_barrier_semaphore()
    for device in (partner, xn, yn):
        pl.semaphore_signal(barrier, inc=1, device_id={"grp": device}, device_id_type=MESH)

    row = lax.broadcasted_iota(jnp.int32, (part, k), 0)
    lane = lax.broadcasted_iota(jnp.int32, (k, part), 1)

    def build_w(q):
        for other in (0, 1):
            shifted = row + base(q, other)
            for g in range(grids):
                value = coef_ref[g].astype(F32)
                hit = ids_ref[g:g + 1, :] == shifted
                w[other * part:(other + 1) * part, g * k:(g + 1) * k] = jnp.where(hit, value, 0.0).astype(BF16)

    def build_oh(q):
        for other in (0, 1):
            shifted = lane + base(q, other)
            for g in range(grids):
                hit = idst[:, g:g + 1] == shifted
                oh[q, g * k:(g + 1) * k, other * part:(other + 1) * part] = jnp.where(hit, 1.0, 0.0).astype(BF16)

    def partial(q):
        p[q] = jnp.dot(w[...], xhi[...], preferred_element_type=F32) + jnp.dot(
            w[...], xlo[...], preferred_element_type=F32)

    started = []
    counter = [0]

    def send(src, dst, device):
        n = counter[0]
        counter[0] += 1
        copy = pltpu.make_async_remote_copy(
            src_ref=src, dst_ref=dst, send_sem=ss.at[n], recv_sem=rs.at[n],
            device_id={"grp": device}, device_id_type=MESH)
        copy.start()
        started.append(copy)
        return copy

    build_w(DIAG)
    for n, copy in enumerate(loads):
        copy.wait()
        for g in range(n * per, (n + 1) * per):
            value = xf[g]
            high = value.astype(BF16)
            xhi[g * k:(g + 1) * k, :] = high
            xlo[g * k:(g + 1) * k, :] = (value - high.astype(F32)).astype(BF16)

    pl.semaphore_wait(barrier, 3)

    def pair(q):
        return send(p.at[q, pl.ds(part, part)], rd.at[q], partner)

    def add_pair(q, copy):
        copy.wait_recv()
        p[q, 0:part] = p[q, 0:part] + rd[q]

    def piece(ref, q, s, half):
        return ref.at[q, pl.ds(s * rows + half * h, h)]

    partial(DIAG)
    pair_d = pair(DIAG)
    build_w(XN)
    partial(XN)
    pair_x = pair(XN)
    add_pair(DIAG, pair_d)
    relay_x, relay_y = [], []
    for s in range(STREAMS):
        relay_x.append(send(piece(p, DIAG, s, 0), rrel.at[0, s], xn))
        relay_y.append(send(piece(p, DIAG, s, 1), rrel.at[1, s], yn))
    build_w(YN)
    partial(YN)
    pair_y = pair(YN)
    add_pair(XN, pair_x)
    plain_x, plain_y, rich_x, rich_y = {}, {}, {}, {}
    plain_x[0] = send(piece(p, XN, 0, 0), rx.at[0, pl.ds(0, h)], xn)
    build_w(OWN)
    add_pair(YN, pair_y)
    plain_y[0] = send(piece(p, YN, 0, 1), ry.at[0, pl.ds(h, h)], yn)
    partial(OWN)
    pair_o = pair(OWN)

    def enrich(s):
        relay_y[s].wait_recv()
        at = s * rows + h
        p[XN, at:at + h] = p[XN, at:at + h] + rrel[1, s]
        rich_x[s] = send(piece(p, XN, s, 1), rx.at[s, pl.ds(h, h)], xn)
        relay_x[s].wait_recv()
        at = s * rows
        p[YN, at:at + h] = p[YN, at:at + h] + rrel[0, s]
        rich_y[s] = send(piece(p, YN, s, 0), ry.at[s, pl.ds(0, h)], yn)

    enrich(0)
    for s in range(1, STREAMS):
        plain_x[s] = send(piece(p, XN, s, 0), rx.at[s, pl.ds(0, h)], xn)
        plain_y[s] = send(piece(p, YN, s, 1), ry.at[s, pl.ds(h, h)], yn)
        enrich(s)
    add_pair(OWN, pair_o)

    padded = jnp.concatenate([ids_ref[...], jnp.zeros((k - grids, k), jnp.int32)], axis=0)
    idst[...] = padded.T
    build_oh(OWN)
    build_oh(XN)
    build_oh(YN)
    build_oh(DIAG)

    def mine(q, s, half):
        return cc.at[q, 0, pl.ds(s * rows + half * h, h)]

    got = {}
    to_partner = {q: [] for q in range(4)}

    def forward(q, s, half):
        span = pl.ds(s * rows + half * h, h)
        to_partner[q].append(send(cc.at[q, 0, span], cc.at[q, 1, span], partner))

    for s in range(STREAMS):
        for copy in (plain_x[s], plain_y[s], rich_x[s], rich_y[s]):
            copy.wait_recv()
        at = s * rows
        cc[OWN, 0, at:at + rows] = p[OWN, at:at + rows] + rx[s] + ry[s]
        for half in (0, 1):
            got[XN, s, half] = send(mine(OWN, s, half), mine(XN, s, half), xn)
            got[YN, s, 1 - half] = send(mine(OWN, s, 1 - half), mine(YN, s, 1 - half), yn)
        span = pl.ds(at, rows)
        to_partner[OWN].append(send(cc.at[OWN, 0, span], cc.at[OWN, 1, span], partner))

    def gather(q, first):
        for copy in to_partner[q]:
            copy.wait_recv()
        for other in (0, 1):
            value = cc[q, other]
            high = value.astype(BF16)
            chi[other * part:(other + 1) * part] = high
            clo[other * part:(other + 1) * part] = (value - high.astype(F32)).astype(BF16)
        found = jnp.dot(oh[q], chi[...], preferred_element_type=F32) + jnp.dot(
            oh[q], clo[...], preferred_element_type=F32)
        found = found.reshape(grids, k, blk)
        out_ref[...] = found if first else out_ref[...] + found

    gather(OWN, True)
    for s in range(STREAMS):
        got[XN, s, 0].wait_recv()
        got[DIAG, s, 0] = send(mine(XN, s, 0), mine(DIAG, s, 0), yn)
        got[YN, s, 1].wait_recv()
        got[DIAG, s, 1] = send(mine(YN, s, 1), mine(DIAG, s, 1), xn)
        forward(XN, s, 0)
        forward(YN, s, 1)
        got[XN, s, 1].wait_recv()
        forward(XN, s, 1)
        got[YN, s, 0].wait_recv()
        forward(YN, s, 0)
    gather(XN, False)
    gather(YN, False)
    for s in range(STREAMS):
        for half in (0, 1):
            got[DIAG, s, half].wait_recv()
            forward(DIAG, s, half)
    gather(DIAG, False)
    for copy in started:
        copy.wait_send()


def square(surplus, block_ids, coef):
    grids, k, blk = surplus.shape
    part = NBD // (SIDE * SIDE * CORES)
    rows = part // STREAMS
    h = rows // 2
    slots = grids * k
    copies = 4 + 6 * STREAMS + 4 * STREAMS + STREAMS + 2 * STREAMS + 6 * STREAMS
    vmem = pl.BlockSpec(memory_space=pltpu.VMEM)
    return pl.pallas_call(
        kernel,
        out_shape=jax.ShapeDtypeStruct(surplus.shape, F32),
        in_specs=[vmem, pl.BlockSpec(memory_space=pltpu.SMEM), pl.BlockSpec(memory_space=pl.ANY)],
        out_specs=vmem,
        scratch_shapes=[
            pltpu.VMEM((grids, k, blk), F32),
            pltpu.VMEM((slots, blk), BF16),
            pltpu.VMEM((slots, blk), BF16),
            pltpu.VMEM((CORES * part, slots), BF16),
            pltpu.VMEM((4, slots, CORES * part), BF16),
            pltpu.VMEM((4, CORES * part, blk), F32),
            pltpu.VMEM((4, part, blk), F32),
            pltpu.VMEM((2, STREAMS, h, blk), F32),
            pltpu.VMEM((STREAMS, rows, blk), F32),
            pltpu.VMEM((STREAMS, rows, blk), F32),
            pltpu.VMEM((4, CORES, part, blk), F32),
            pltpu.VMEM((CORES * part, blk), BF16),
            pltpu.VMEM((CORES * part, blk), BF16),
            pltpu.VMEM((k, k), jnp.int32),
            pltpu.SemaphoreType.DMA((LOADS,)),
            pltpu.SemaphoreType.DMA((copies,)),
            pltpu.SemaphoreType.DMA((copies,)),
        ],
        compiler_params=pltpu.CompilerParams(
            collective_id=0, has_side_effects=True, vmem_limit_bytes=56 * 2**20),
    )(block_ids, coef, surplus)


def local(surplus, block_ids, coef):
    offset = lax.axis_index("dom") * NBD
    local_ids = block_ids - offset
    columns = lax.broadcasted_iota(jnp.int32, (1, 1, NBD), 2)
    onehot = (local_ids[:, :, None] == columns).astype(jnp.float32)
    scaled = surplus * coef.astype(jnp.float32)[:, None, None]
    partial_sum = jnp.einsum("gkn,gkb->nb", onehot, scaled, precision=lax.Precision.HIGHEST)
    combined = lax.psum(partial_sum, "grp")
    return jnp.einsum("gkn,nb->gkb", onehot, combined, precision=lax.Precision.HIGHEST)


def solution(mesh):
    body = square if mesh.shape["grp"] == SIDE * SIDE * CORES else local
    return jax.shard_map(
        body,
        mesh=mesh,
        in_specs=(P("grp", "dom", None), P("grp", "dom"), P("grp")),
        out_specs=P("grp", "dom", None),
        check_vma=False,
    )
```

```python
import functools

import jax
import jax.numpy as jnp
from jax import lax
from jax.experimental import pallas as pl
from jax.experimental.pallas import tpu as pltpu
from jax.sharding import PartitionSpec as P

NBD = 1024
CORES = 2
SIDE = 2
STREAMS = 2
LOADS = 4
MESH = pl.DeviceIdType.MESH
DIAG, XN, YN, OWN = 0, 1, 2, 3
F32, BF16 = jnp.float32, jnp.bfloat16


def kernel(ids_ref, coef_ref, x_ref, out_ref, xf, xhi, xlo, w, oh, p, rd, rrel,
           rx, ry, cc, chl, idst, load_sem, ss, rs):
    grids, k, blk = x_ref.shape
    part = rd.shape[1]
    rows = part // STREAMS
    h = rows // 2
    per = grids // LOADS

    me = lax.axis_index("grp")
    core = lax.rem(me, CORES)
    chip = me // CORES
    x, y = lax.rem(chip, SIDE), chip // SIDE
    ox, oy = 1 - x, 1 - y

    def index_of(cy, cx):
        return cy * SIDE + cx

    chips = {DIAG: index_of(oy, ox), XN: index_of(y, ox), YN: index_of(oy, x), OWN: chip}
    partner = chip * CORES + (1 - core)
    xn, yn = chips[XN] * CORES + core, chips[YN] * CORES + core
    origin = lax.axis_index("dom") * NBD

    def base(q, other):
        c = 1 - core if other else core
        return origin + (chips[q] * CORES + c) * part

    loads = []
    for n in range(LOADS):
        span = pl.ds(n * per, per)
        copy = pltpu.make_async_copy(x_ref.at[span], xf.at[span], load_sem.at[n])
        copy.start()
        loads.append(copy)

    barrier = pltpu.get_barrier_semaphore()
    for device in (partner, xn, yn):
        pl.semaphore_signal(barrier, inc=1, device_id={"grp": device}, device_id_type=MESH)

    row = lax.broadcasted_iota(jnp.int32, (part, k), 0)
    lane = lax.broadcasted_iota(jnp.int32, (k, 2 * rows), 1)

    def build_w(q):
        for other in (0, 1):
            shifted = row + base(q, other)
            for g in range(grids):
                value = coef_ref[g].astype(F32)
                hit = ids_ref[g:g + 1, :] == shifted
                w[other * part:(other + 1) * part, g * k:(g + 1) * k] = jnp.where(hit, value, 0.0).astype(BF16)

    def build_oh(q):
        for s in range(STREAMS):
            start = jnp.where(lane < rows, base(q, 0), base(q, 1) - rows) + s * rows
            shifted = lane + start
            for g in range(grids):
                hit = jnp.where(idst[:, g:g + 1] == shifted, 1.0, 0.0).astype(BF16)
                oh[q, s, g * k:(g + 1) * k, 0:2 * rows] = hit
                oh[q, s, g * k:(g + 1) * k, 2 * rows:4 * rows] = hit

    def half_of(q, other):
        at = other * part
        p[q, at:at + part] = jnp.dot(w[at:at + part], xhi[...], preferred_element_type=F32) + jnp.dot(
            w[at:at + part], xlo[...], preferred_element_type=F32)

    started = []
    counter = [0]

    def send(src, dst, device):
        n = counter[0]
        counter[0] += 1
        copy = pltpu.make_async_remote_copy(
            src_ref=src, dst_ref=dst, send_sem=ss.at[n], recv_sem=rs.at[n],
            device_id={"grp": device}, device_id_type=MESH)
        copy.start()
        started.append(copy)
        return copy

    build_w(DIAG)
    for n, copy in enumerate(loads):
        copy.wait()
        for g in range(n * per, (n + 1) * per):
            value = xf[g]
            high = value.astype(BF16)
            xhi[g * k:(g + 1) * k, :] = high
            xlo[g * k:(g + 1) * k, :] = (value - high.astype(F32)).astype(BF16)
        lo, hi = n * per * k, (n + 1) * per * k
        if n < LOADS - 1:
            term = jnp.dot(w[:, lo:hi], xhi[lo:hi], preferred_element_type=F32) + jnp.dot(
                w[:, lo:hi], xlo[lo:hi], preferred_element_type=F32)
            p[DIAG] = term if n == 0 else p[DIAG] + term

    pl.semaphore_wait(barrier, 3)

    def last_term(other):
        at, lo = other * part, (LOADS - 1) * per * k
        p[DIAG, at:at + part] = p[DIAG, at:at + part] + (
            jnp.dot(w[at:at + part, lo:], xhi[lo:], preferred_element_type=F32) + jnp.dot(
                w[at:at + part, lo:], xlo[lo:], preferred_element_type=F32))

    def pair(q):
        return send(p.at[q, pl.ds(part, part)], rd.at[q], partner)

    def add_pair(q, copy):
        copy.wait_recv()
        p[q, 0:part] = p[q, 0:part] + rd[q]

    def piece(ref, q, s, half):
        return ref.at[q, pl.ds(s * rows + half * h, h)]

    def enrich(s):
        relay_y[s].wait_recv()
        at = s * rows + h
        p[XN, at:at + h] = p[XN, at:at + h] + rrel[1, s]
        rich_x[s] = send(piece(p, XN, s, 1), rx.at[s, pl.ds(h, h)], xn)
        relay_x[s].wait_recv()
        at = s * rows
        p[YN, at:at + h] = p[YN, at:at + h] + rrel[0, s]
        rich_y[s] = send(piece(p, YN, s, 0), ry.at[s, pl.ds(0, h)], yn)

    last_term(1)
    pair_d = [send(p.at[DIAG, pl.ds(part + s * rows, rows)], rd.at[DIAG, pl.ds(s * rows, rows)], partner)
              for s in range(STREAMS)]
    last_term(0)
    build_w(XN)
    half_of(XN, 1)
    pair_x = pair(XN)
    relay_x, relay_y = [], []
    for s in range(STREAMS):
        pair_d[s].wait_recv()
        at = s * rows
        p[DIAG, at:at + rows] = p[DIAG, at:at + rows] + rd[DIAG, at:at + rows]
        relay_x.append(send(piece(p, DIAG, s, 0), rrel.at[0, s], xn))
        relay_y.append(send(piece(p, DIAG, s, 1), rrel.at[1, s], yn))
    plain_x, plain_y, rich_x, rich_y = {}, {}, {}, {}
    half_of(XN, 0)
    add_pair(XN, pair_x)
    plain_x[0] = send(piece(p, XN, 0, 0), rx.at[0, pl.ds(0, h)], xn)
    build_w(YN)
    half_of(YN, 1)
    pair_y = pair(YN)
    half_of(YN, 0)
    add_pair(YN, pair_y)
    plain_y[0] = send(piece(p, YN, 0, 1), ry.at[0, pl.ds(h, h)], yn)
    build_w(OWN)
    enrich(0)
    pair_o = None
    for s in range(1, STREAMS):
        plain_x[s] = send(piece(p, XN, s, 0), rx.at[s, pl.ds(0, h)], xn)
        plain_y[s] = send(piece(p, YN, s, 1), ry.at[s, pl.ds(h, h)], yn)
        if s == 1:
            half_of(OWN, 1)
            pair_o = pair(OWN)
            half_of(OWN, 0)
        enrich(s)
    add_pair(OWN, pair_o)

    padded = jnp.concatenate([ids_ref[...], jnp.zeros((k - grids, k), jnp.int32)], axis=0)
    idst[...] = padded.T
    build_oh(OWN)
    build_oh(XN)
    build_oh(YN)

    def mine(q, s, half):
        return cc.at[q, 0, pl.ds(s * rows + half * h, h)]

    got = {}
    to_partner = {(q, s): [] for q in range(4) for s in range(STREAMS)}

    def forward(q, s, half):
        span = pl.ds(s * rows + half * h, h)
        to_partner[q, s].append(send(cc.at[q, 0, span], cc.at[q, 1, span], partner))

    for s in range(STREAMS):
        for copy in (plain_x[s], plain_y[s], rich_x[s], rich_y[s]):
            copy.wait_recv()
        at = s * rows
        cc[OWN, 0, at:at + rows] = p[OWN, at:at + rows] + rx[s] + ry[s]
        for half in (0, 1):
            got[XN, s, half] = send(mine(OWN, s, half), mine(XN, s, half), xn)
            got[YN, s, 1 - half] = send(mine(OWN, s, 1 - half), mine(YN, s, 1 - half), yn)
        span = pl.ds(at, rows)
        to_partner[OWN, s].append(send(cc.at[OWN, 0, span], cc.at[OWN, 1, span], partner))

    build_oh(DIAG)

    def gather(q, s, first=False):
        for copy in to_partner[q, s]:
            copy.wait_recv()
        for other in (0, 1):
            value = cc[q, other, s * rows:(s + 1) * rows]
            high = value.astype(BF16)
            at = other * rows
            chl[at:at + rows] = high
            chl[2 * rows + at:3 * rows + at] = (value - high.astype(F32)).astype(BF16)
        found = jnp.dot(oh[q, s], chl[...], preferred_element_type=F32).reshape(grids, k, blk)
        out_ref[...] = found if first else out_ref[...] + found

    for s in range(STREAMS):
        gather(OWN, s, s == 0)
    for s in range(STREAMS):
        got[XN, s, 0].wait_recv()
        got[DIAG, s, 0] = send(mine(XN, s, 0), mine(DIAG, s, 0), yn)
        got[YN, s, 1].wait_recv()
        got[DIAG, s, 1] = send(mine(YN, s, 1), mine(DIAG, s, 1), xn)
        forward(XN, s, 0)
        forward(YN, s, 1)
        got[XN, s, 1].wait_recv()
        forward(XN, s, 1)
        got[YN, s, 0].wait_recv()
        forward(YN, s, 0)
        if s < STREAMS - 1:
            gather(XN, s)
            gather(YN, s)
    gather(XN, STREAMS - 1)
    for s in range(STREAMS):
        for half in (0, 1):
            got[DIAG, s, half].wait_recv()
            forward(DIAG, s, half)
        if s == 0:
            gather(YN, STREAMS - 1)
        gather(DIAG, s)
    for copy in started:
        copy.wait_send()


def square(surplus, block_ids, coef):
    grids, k, blk = surplus.shape
    part = NBD // (SIDE * SIDE * CORES)
    rows = part // STREAMS
    h = rows // 2
    slots = grids * k
    copies = 3 + STREAMS + 6 * STREAMS + 4 * STREAMS + STREAMS + 2 * STREAMS + 6 * STREAMS
    vmem = pl.BlockSpec(memory_space=pltpu.VMEM)
    return pl.pallas_call(
        kernel,
        out_shape=pltpu.VMEM(surplus.shape, F32),
        in_specs=[vmem, pl.BlockSpec(memory_space=pltpu.SMEM), pl.BlockSpec(memory_space=pl.ANY)],
        out_specs=vmem,
        scratch_shapes=[
            pltpu.VMEM((grids, k, blk), F32),
            pltpu.VMEM((slots, blk), BF16),
            pltpu.VMEM((slots, blk), BF16),
            pltpu.VMEM((CORES * part, slots), BF16),
            pltpu.VMEM((4, STREAMS, slots, 4 * rows), BF16),
            pltpu.VMEM((4, CORES * part, blk), F32),
            pltpu.VMEM((4, part, blk), F32),
            pltpu.VMEM((2, STREAMS, h, blk), F32),
            pltpu.VMEM((STREAMS, rows, blk), F32),
            pltpu.VMEM((STREAMS, rows, blk), F32),
            pltpu.VMEM((4, CORES, part, blk), F32),
            pltpu.VMEM((4 * rows, blk), BF16),
            pltpu.VMEM((k, k), jnp.int32),
            pltpu.SemaphoreType.DMA((LOADS,)),
            pltpu.SemaphoreType.DMA((copies,)),
            pltpu.SemaphoreType.DMA((copies,)),
        ],
        compiler_params=pltpu.CompilerParams(
            collective_id=0, has_side_effects=True, vmem_limit_bytes=56 * 2**20),
    )(block_ids, coef, surplus)


def local(surplus, block_ids, coef):
    offset = lax.axis_index("dom") * NBD
    local_ids = block_ids - offset
    columns = lax.broadcasted_iota(jnp.int32, (1, 1, NBD), 2)
    onehot = (local_ids[:, :, None] == columns).astype(jnp.float32)
    scaled = surplus * coef.astype(jnp.float32)[:, None, None]
    partial_sum = jnp.einsum("gkn,gkb->nb", onehot, scaled, precision=lax.Precision.HIGHEST)
    combined = lax.psum(partial_sum, "grp")
    return jnp.einsum("gkn,nb->gkb", onehot, combined, precision=lax.Precision.HIGHEST)


def solution(mesh):
    body = square if mesh.shape["grp"] == SIDE * SIDE * CORES else local
    return jax.shard_map(
        body,
        mesh=mesh,
        in_specs=(P("grp", "dom", None), P("grp", "dom"), P("grp")),
        out_specs=P("grp", "dom", None),
        check_vma=False,
    )
```
